32 devices in a mesh: tm: 8 (over y, x, core), panel: 4 (over z).
Axes of the slice: x: 2, y: 2, z: 4, core: 2. Of those that a mesh axis runs over, the one named last changes fastest.
Arguments:
- observed: bfloat16 [4096, 4096], P('tm', 'panel'), may hold values from -12 to 12
- present: int32 [32, 4096], P('tm', 'panel'), may hold values 0 or 1
- loadings: bfloat16 [4096, 256], P('panel'), may hold values from -0.09375 to 0.09375
- noise_var: float32 [4096], P('panel'), may hold values from 1 to 4
- decay_rate: float32 [256], replicated, may hold values from 2.4414063e-05 to 0.03
- panel_of_block: int32 [32], P('panel'), may hold values from 0 to 18
Outputs:
- smoothed: float32 [4096, 256], P('tm')
- loading_moment: float32 [256, 4096], P('tm', 'panel')
- state_moment: float32 [256, 256], replicated
- panel_var: float32 [19], replicated
The draws below stay inside these ranges and needn't reach their ends.
All inputs are finite; a program needn't handle non-finite values. No bound on the sum of `present` on one device may be relied on, other than what follows from the above.
Results may differ from the reference program's by a relative error of at most 0.00055.
Values sent between devices are 32-bit elements; how exact they have to be, the bound alone decides.
A program may use at most 128 MiB of HBM per device.

```python
import math
import jax
import jax.numpy as jnp
from jax import lax

S = 256
P_SIZE = 4096
SER_BLOCK = 128
PANELS = 19
BLOCK = 128
TIME = 4096
NB_ALL = 32


def loading_table(key):
    key_pick, key_scale, key_values = jax.random.split(key, 3)
    order = jax.random.permutation(key_pick, S)
    strong = order < S // 2
    spread = jax.random.uniform(key_scale, (S,), jnp.float32, 0.0, 1.0)
    column_scale = jnp.where(strong, 0.25 * 4.0 ** spread, 0.004 * 4.0 ** spread)
    values = jax.random.truncated_normal(key_values, -5.9, 5.9, (P_SIZE, S), jnp.float32)
    return values * column_scale[None, :] * P_SIZE ** (-0.5)


def draw_loadings(key, part):
    return loading_table(jax.random.fold_in(key, 101)).astype(jnp.bfloat16)


def draw_observed(key, part):
    loads = loading_table(jax.random.fold_in(key, 101)).astype(jnp.bfloat16).astype(jnp.float32)
    key_rate, key_start, key_steps, key_noise = jax.random.split(jax.random.fold_in(key, 202), 4)
    rate = 0.002 * 10.0 ** jax.random.uniform(key_rate, (S,), jnp.float32, 0.0, 1.0)
    amplitude = 4.0
    keep = 1.0 - rate
    kick = amplitude * jnp.sqrt(1.0 - keep * keep)
    start = amplitude * jax.random.normal(key_start, (S,), jnp.float32)
    shocks = jax.random.normal(key_steps, (TIME, S), jnp.float32)

    def advance(state, shock_row):
        following = keep * state + kick * shock_row
        return (following, following)
    unused_state, factors = lax.scan(advance, start, shocks)
    noise = jax.random.truncated_normal(key_noise, -6.0, 6.0, (TIME, P_SIZE), jnp.float32)
    signal = jnp.dot(factors, loads.T, precision=lax.Precision.HIGHEST)
    return jnp.clip(signal + noise, -12.0, 12.0).astype(jnp.bfloat16)


def place_ends(drawn, key, smallest, largest):
    longest = drawn.shape.index(max(drawn.shape))
    spots = []
    for shift in (0, 1):
        where = [jax.random.randint(jax.random.fold_in(key, axis), (), 0, length) for axis, length in enumerate(drawn.shape)]
        where[longest] = (where[longest] + shift) % drawn.shape[longest]
        spots.append(tuple(where))
    return drawn.at[spots[0]].set(smallest).at[spots[1]].set(largest)


def block_scale(stream_key, shape, pieces, least, high):
    gain = 1.0
    for dim, shards_of in pieces:
        draws = jax.random.uniform(jax.random.fold_in(jax.random.fold_in(stream_key, 6), dim), (shards_of,), jnp.float32, least / len(pieces), high / len(pieces))
        gain = gain * jnp.repeat(jnp.exp(draws), shape[dim] // shards_of).reshape((-1,) + (1,) * (len(shape) - 1 - dim))
    return gain


def setup_inputs(seed: int = 0) -> dict:
    key_of = jax.random.split(jax.random.key(seed), 7)
    observed = draw_observed(jax.random.fold_in(key_of[6], 71), 0)
    present = place_ends((jax.random.randint(key_of[1], (NB_ALL, P_SIZE), 0, 4) < 3).astype(jnp.int32), jax.random.fold_in(key_of[1], 1), 0, 1)
    loadings = draw_loadings(jax.random.fold_in(key_of[6], 71), 0)
    noise_var = jnp.clip(jnp.exp(math.log(4.0) - 1.3862944 * jax.random.uniform(key_of[3], (P_SIZE,), jnp.float32) ** block_scale(key_of[3], (P_SIZE,), ((0, 4),), -0.2, 0.2)), 1.0, 4.0)
    decay_rate = jnp.clip(jnp.exp(jax.random.uniform(key_of[4], (S,), jnp.float32, math.log(2.441406286379788e-05), math.log(0.03))), 2.441406286379788e-05, 0.03)
    panel_of_block = place_ends(jax.random.randint(key_of[5], (P_SIZE // SER_BLOCK,), 0, PANELS), jax.random.fold_in(key_of[5], 1), 0, PANELS - 1).astype(jnp.int32)
    return {"observed": observed, "present": present, "loadings": loadings, "noise_var": noise_var, "decay_rate": decay_rate, "panel_of_block": panel_of_block}


HIGH = lax.Precision.HIGHEST

def invert_one(gram_block):
    identity = jnp.eye(S, dtype=jnp.float32)
    factor = jnp.linalg.cholesky(identity + gram_block)
    return jax.scipy.linalg.cho_solve((factor, True), identity)

def reference(observed, present, loadings, noise_var, decay_rate, panel_of_block):
    loads = loadings.astype(jnp.float32)
    inv_noise = 1.0 / noise_var
    kept_mask = present.astype(jnp.float32)
    weighted = loads * inv_noise[:, None]

    def gram_one(mask_row):
        return jnp.dot((weighted * mask_row[:, None]).T, loads, precision=HIGH)
    gram_sum = lax.map(gram_one, kept_mask)
    inverse = lax.map(invert_one, gram_sum)
    persist = 1.0 - decay_rate
    transit = inverse * persist[None, None, :]
    obs_kept = observed.astype(jnp.float32).reshape(NB_ALL, BLOCK, P_SIZE) * kept_mask[:, None, :]
    projected = jnp.dot((obs_kept * inv_noise).reshape(TIME, P_SIZE), loads, precision=HIGH)
    inputs = jnp.einsum('bts,brs->btr', projected.reshape(NB_ALL, BLOCK, S), inverse, precision=HIGH)

    def run_block(state, block_pair):
        matrix, block_rows = block_pair

        def advance(carried, input_row):
            following = jnp.dot(matrix, carried, precision=HIGH) + input_row
            return (following, following)
        return lax.scan(advance, state, block_rows, reverse=False)

    def run_block_back(state, block_pair):
        matrix, block_rows = block_pair

        def advance(carried, input_row):
            following = jnp.dot(matrix, carried, precision=HIGH) + input_row
            return (following, following)
        return lax.scan(advance, state, block_rows, reverse=True)
    start_state = jnp.zeros((S,), jnp.float32)
    final_state, filtered = lax.scan(run_block, start_state, (transit, inputs))
    offsets = filtered - jnp.einsum('btr,bsr->bts', filtered * persist, transit, precision=HIGH)
    offsets = offsets.at[-1, -1].set(filtered[-1, -1])
    first_state, smooth_rows = lax.scan(run_block_back, start_state, (transit, offsets), reverse=True)
    smoothed = smooth_rows.reshape(TIME, S)
    state_moment = jnp.dot(smoothed.T, smoothed, precision=HIGH) / TIME
    flat_kept = obs_kept.reshape(TIME, P_SIZE)
    loading_moment = jnp.dot(smoothed.T, flat_kept, precision=HIGH) / math.sqrt(TIME)
    fitted = jnp.dot(smoothed, loads.T, precision=HIGH).reshape(NB_ALL, BLOCK, P_SIZE) * kept_mask[:, None, :]
    errors = obs_kept - fitted
    square_sums = lax.optimization_barrier(jnp.sum(errors * errors, axis=(0, 1)))
    obs_counts = BLOCK * lax.optimization_barrier(jnp.sum(kept_mask, axis=0))
    onehot = (panel_of_block[:, None] == jnp.arange(PANELS, dtype=jnp.int32)[None, :]).astype(jnp.float32)
    panel_sums = jnp.dot(square_sums.reshape(-1, SER_BLOCK).sum(axis=1), onehot, precision=HIGH)
    panel_counts = jnp.dot(obs_counts.reshape(-1, SER_BLOCK).sum(axis=1), onehot, precision=HIGH)
    panel_var = panel_sums / jnp.maximum(panel_counts, 1.0)
    return (smoothed, loading_moment, state_moment, panel_var)
```

```python
import functools
import math

import jax
import jax.numpy as jnp
from jax import lax
from jax.experimental import pallas as pl
from jax.experimental.pallas import tpu as pltpu
from jax.sharding import PartitionSpec as P

SER_BLOCK = 128
PANELS = 19
LEVELS = 7
BLOCK = 128
PAD = 8

HIGH = lax.Precision.HIGHEST
MESH = pl.DeviceIdType.MESH
VMEM_LIMIT = 60 * 1024 * 1024


def mm(a, b):
    return jnp.dot(a, b, precision=HIGH, preferred_element_type=jnp.float32)


def mm_t(a, b):
    return lax.dot_general(
        a, b, (((1,), (1,)), ((), ())), precision=HIGH, preferred_element_type=jnp.float32
    )


def vmem(n):
    return [pl.BlockSpec(memory_space=pltpu.VMEM)] * n


def params(collective_id=None):
    if collective_id is None:
        return pltpu.CompilerParams(vmem_limit_bytes=VMEM_LIMIT)
    return pltpu.CompilerParams(
        vmem_limit_bytes=VMEM_LIMIT, collective_id=collective_id, has_side_effects=True
    )


def send_all(axis, n, me, source, target, send, recv):
    def one(d, unused):
        peer = lax.rem(me + d, n)
        pltpu.make_async_remote_copy(
            src_ref=source(peer),
            dst_ref=target(me, d),
            send_sem=send.at[d - 1],
            recv_sem=recv.at[d - 1],
            device_id={axis: peer},
            device_id_type=MESH,
        ).start()
        return unused

    lax.fori_loop(1, n, one, 0)


def wait_all(axis, n, me, source, target, send, recv):
    def one(d, unused):
        origin = lax.rem(me + n - d, n)
        copy = pltpu.make_async_remote_copy(
            src_ref=source(lax.rem(me + d, n)),
            dst_ref=target(origin, d),
            send_sem=send.at[d - 1],
            recv_sem=recv.at[d - 1],
            device_id={axis: origin},
            device_id_type=MESH,
        )
        copy.wait_recv()
        copy.wait_send()
        return unused

    lax.fori_loop(1, n, one, 0)


def greet(groups):
    barrier = pltpu.get_barrier_semaphore()
    total = 0
    for axis, n, me in groups:

        def one(d, unused, axis=axis, n=n, me=me):
            pl.semaphore_signal(
                barrier, inc=1, device_id={axis: lax.rem(me + d, n)}, device_id_type=MESH
            )
            return unused

        lax.fori_loop(1, n, one, 0)
        total += n - 1
    pl.semaphore_wait(barrier, total)


def scatter_kernel(panels, parts, out, landed, send, recv):
    me = lax.axis_index("panel")
    greet([("panel", panels, me)])
    args = ("panel", panels, me, lambda peer: parts.at[peer], lambda i, d: landed.at[d - 1])
    send_all(*args, send, recv)
    total = parts[me]
    wait_all(*args, send, recv)
    for d in range(panels - 1):
        total = total + landed[d]
    out[...] = total


def scatter_panel(parts):
    panels = parts.shape[0]
    shape = parts.shape[1:]
    return pl.pallas_call(
        functools.partial(scatter_kernel, panels),
        out_shape=jax.ShapeDtypeStruct(shape, jnp.float32),
        in_specs=vmem(1),
        out_specs=pl.BlockSpec(memory_space=pltpu.VMEM),
        scratch_shapes=[
            pltpu.VMEM((panels - 1,) + shape, jnp.float32),
            pltpu.SemaphoreType.DMA((panels - 1,)),
            pltpu.SemaphoreType.DMA((panels - 1,)),
        ],
        compiler_params=params(1),
        name="scatter_panel",
    )(parts)


def shift_rows(moved, offset, ahead):
    rows = moved.shape[0]
    zero = jnp.zeros((offset, moved.shape[1]), jnp.float32)
    if offset % 8 == 0:
        if ahead:
            return jnp.concatenate([zero, moved[: rows - offset]], axis=0)
        return jnp.concatenate([moved[offset:], zero], axis=0)
    row = lax.broadcasted_iota(jnp.int32, moved.shape, 0)
    if ahead:
        return jnp.where(row >= offset, pltpu.roll(moved, offset, 0), 0.0)
    return jnp.where(row < rows - offset, pltpu.roll(moved, rows - offset, 0), 0.0)


def local_kernel(reduced, rho, pack, powers, values_out, stack):
    width = reduced.shape[1]
    gram = reduced[:width]
    eye = (
        lax.broadcasted_iota(jnp.int32, (width, width), 0)
        == lax.broadcasted_iota(jnp.int32, (width, width), 1)
    ).astype(jnp.float32)
    bound = jnp.max(jnp.sum(jnp.abs(gram), axis=1))
    alpha = 2.0 / (2.0 + bound)
    rest = eye - alpha * (eye + gram)
    stack[:width] = eye + rest
    stack[width:] = mm(rest, rest)
    ratio = bound / (2.0 + bound)

    def step(level):
        grown = mm(stack[...], stack[width:])
        stack[:width] = stack[:width] + grown[:width]
        stack[width:] = grown[width:]
        return level * level

    lax.while_loop(lambda level: level > 1e-5, step, ratio * ratio)
    guess = alpha * stack[:width]
    inverse = guess + mm(guess, (eye - guess) - mm(gram, guess))
    values = mm(reduced[width:], inverse)
    power = rho[...] * inverse
    for level in range(LEVELS):
        powers[level] = power
        both = mm(jnp.concatenate([power, values], axis=0), power)
        values = values + shift_rows(both[width:], 1 << level, True)
        power = both[:width]
    values_out[...] = values
    pack[:width] = power
    row = lax.broadcasted_iota(jnp.int32, (PAD, width), 0)
    pack[width:] = jnp.where(row == 0, pltpu.roll(values[BLOCK - PAD :], 1, 0), 0.0)


def local_tables(reduced, persist):
    width = reduced.shape[1]
    f32 = jnp.float32
    return pl.pallas_call(
        local_kernel,
        out_shape=(
            jax.ShapeDtypeStruct((width + PAD, width), f32),
            jax.ShapeDtypeStruct((LEVELS, width, width), f32),
            jax.ShapeDtypeStruct((BLOCK, width), f32),
        ),
        in_specs=vmem(2),
        out_specs=tuple(vmem(3)),
        scratch_shapes=[pltpu.VMEM((2 * width, width), f32)],
        compiler_params=params(),
        name="local_tables",
    )(reduced, persist[:, None])


def spread(first, powers, ahead):
    rows = mm(first, powers[0])
    if not ahead:
        rows = pltpu.roll(rows, PAD - 1, 0)
    for level in range(LEVELS):
        moved = mm(rows, powers[level])
        if level < 3:
            offset = 1 << level
            rows = rows + pltpu.roll(moved, offset if ahead else PAD - offset, 0)
        elif ahead:
            rows = jnp.concatenate([rows, moved], axis=0)
        else:
            rows = jnp.concatenate([moved, rows], axis=0)
    return rows


def smooth_kernel(
    segments,
    panels,
    pack,
    powers,
    partial,
    rho,
    out,
    near,
    far,
    seg_pack,
    own_first,
    firsts,
    seg_first,
    seg_firsts,
    mine,
    near_send,
    near_recv,
    far_send,
    far_recv,
):
    width = pack.shape[1]
    place = lax.axis_index("panel")
    segment = lax.axis_index("tm")
    greet([("panel", panels, place), ("tm", segments, segment)])

    def gather(axis, n, me, source, target, stage):
        send, recv = (near_send, near_recv) if axis == "panel" else (far_send, far_recv)
        args = (axis, n, me, lambda peer: source, lambda i, d: target.at[i])
        send_all(*args, send.at[stage], recv.at[stage])
        target[me] = source[...]
        wait_all(*args, send.at[stage], recv.at[stage])

    row = lax.broadcasted_iota(jnp.int32, (PAD, width), 0)
    decay = rho[...]
    gather("panel", panels, place, pack, near, 0)
    whole = near[0]
    keep = (lax.broadcasted_iota(jnp.int32, (width + PAD, width), 0) >= width).astype(jnp.float32)
    for k in range(1, panels):
        whole = mm(whole, near[k, :width]) + keep * near[k]
    seg_pack[...] = whole
    gather("tm", segments, segment, seg_pack, far, 0)

    def far_ahead(k, state):
        new = mm(state, far[k, :width]) + far[k, width:]
        return jnp.where(k < segment, new, state)

    state = lax.fori_loop(0, segments - 1, far_ahead, jnp.zeros((PAD, width), jnp.float32))
    for k in range(panels - 1):
        state = jnp.where(k < place, mm(state, near[k, :width]) + near[k, width:], state)

    filtered = partial[...] + spread(state, powers, True)
    values = filtered - mm(filtered * decay, powers[0])
    last = jnp.logical_and(segment == segments - 1, place == panels - 1)
    final_row = lax.broadcasted_iota(jnp.int32, (BLOCK, width), 0) == BLOCK - 1
    values = jnp.where(jnp.logical_and(final_row, last), filtered, values)
    for level in range(LEVELS):
        values = values + shift_rows(mm(values, powers[level]), 1 << level, False)
    own_first[...] = jnp.where(row == 0, values[:PAD], 0.0)
    gather("panel", panels, place, own_first, firsts, 1)
    total = firsts[panels - 1]
    for k in range(panels - 2, -1, -1):
        total = mm(total, near[k, :width]) + firsts[k]
    seg_first[...] = total * decay
    gather("tm", segments, segment, seg_first, seg_firsts, 1)

    def far_back(j, state):
        k = segments - 1 - j
        new = mm_t(state, far[k, :width]) + seg_firsts[k]
        return jnp.where(k > segment, new, state)

    state = lax.fori_loop(0, segments - 1, far_back, jnp.zeros((PAD, width), jnp.float32))
    state = state / decay
    for k in range(panels - 1, 0, -1):
        state = jnp.where(k > place, mm(state, near[k, :width]) + firsts[k], state)
    mine[...] = values + spread(state, powers, False)
    gather("panel", panels, place, mine, out, 2)


def smooth(pack, powers, partial, persist):
    width = pack.shape[1]
    segments, panels = lax.axis_size("tm"), lax.axis_size("panel")
    f32 = jnp.float32
    return pl.pallas_call(
        functools.partial(smooth_kernel, segments, panels),
        out_shape=jax.ShapeDtypeStruct((panels, BLOCK, width), f32),
        in_specs=vmem(4),
        out_specs=pl.BlockSpec(memory_space=pltpu.VMEM),
        scratch_shapes=[
            pltpu.VMEM((panels, width + PAD, width), f32),
            pltpu.VMEM((segments, width + PAD, width), f32),
            pltpu.VMEM((width + PAD, width), f32),
            pltpu.VMEM((PAD, width), f32),
            pltpu.VMEM((panels, PAD, width), f32),
            pltpu.VMEM((PAD, width), f32),
            pltpu.VMEM((segments, PAD, width), f32),
            pltpu.VMEM((BLOCK, width), f32),
            pltpu.SemaphoreType.DMA((3, panels - 1)),
            pltpu.SemaphoreType.DMA((3, panels - 1)),
            pltpu.SemaphoreType.DMA((2, segments - 1)),
            pltpu.SemaphoreType.DMA((2, segments - 1)),
        ],
        compiler_params=params(2),
        name="smooth",
    )(pack, powers, partial, persist[None, :])


def finish_kernel(
    segments, panels, cross, moment, sums, out, gathered, landed, moments, bundle, *sems
):
    c_send, c_recv, m_send, m_recv, g_send, g_recv = sems
    place = lax.axis_index("panel")
    segment = lax.axis_index("tm")
    devices = segments * panels
    me = place * segments + segment
    rows = moment.shape[1]
    barrier = pltpu.get_barrier_semaphore()

    def where(d):
        peer = lax.rem(me + d, devices)
        return {"tm": lax.rem(peer, segments), "panel": peer // segments}

    def hello(d, unused):
        pl.semaphore_signal(barrier, inc=1, device_id=where(d), device_id_type=MESH)
        return unused

    lax.fori_loop(1, devices, hello, 0)
    pl.semaphore_wait(barrier, devices - 1)

    m_args = ("tm", segments, segment, lambda i: moment.at[i], lambda i, d: moments.at[d - 1])
    c_args = ("tm", segments, segment, lambda i: cross.at[i], lambda i, d: landed.at[d - 1])
    send_all(*m_args, m_send, m_recv)
    send_all(*c_args, c_send, c_recv)
    own = moment[segment]
    wait_all(*m_args, m_send, m_recv)
    for d in range(segments - 1):
        own = own + moments[d]
    bundle[:rows] = own
    bundle[rows:] = sums[...]
    gathered[me] = bundle[...]

    def copy(d, slot):
        return pltpu.make_async_remote_copy(
            src_ref=bundle,
            dst_ref=gathered.at[slot],
            send_sem=g_send.at[d - 1],
            recv_sem=g_recv.at[d - 1],
            device_id=where(d),
            device_id_type=MESH,
        )

    def push(d, unused):
        copy(d, me).start()
        return unused

    lax.fori_loop(1, devices, push, 0)
    total = cross[segment]
    wait_all(*c_args, c_send, c_recv)
    for d in range(segments - 1):
        total = total + landed[d]
    out[...] = total

    def pull(d, unused):
        got = copy(d, lax.rem(me + devices - d, devices))
        got.wait_recv()
        got.wait_send()
        return unused

    lax.fori_loop(1, devices, pull, 0)


def finish(cross, moment, sums):
    segments, panels = lax.axis_size("tm"), lax.axis_size("panel")
    devices = segments * panels
    f32 = jnp.float32
    rows = moment.shape[1] + sums.shape[0]
    dma = pltpu.SemaphoreType.DMA
    return pl.pallas_call(
        functools.partial(finish_kernel, segments, panels),
        out_shape=(
            jax.ShapeDtypeStruct(cross.shape[1:], f32),
            jax.ShapeDtypeStruct((devices, rows, 128), f32),
        ),
        in_specs=vmem(3),
        out_specs=tuple(vmem(2)),
        scratch_shapes=[
            pltpu.VMEM((segments - 1,) + cross.shape[1:], f32),
            pltpu.VMEM((segments - 1,) + moment.shape[1:], f32),
            pltpu.VMEM((rows, 128), f32),
            dma((segments - 1,)),
            dma((segments - 1,)),
            dma((segments - 1,)),
            dma((segments - 1,)),
            dma((devices - 1,)),
            dma((devices - 1,)),
        ],
        compiler_params=params(3),
        name="finish",
    )(cross, moment, sums)


def per_device(observed, present, loadings, noise_var, decay_rate, panel_of_block):
    time_rows, series = observed.shape
    width = loadings.shape[1]
    nblocks = time_rows // BLOCK
    segments, panels = lax.axis_size("tm"), lax.axis_size("panel")
    assert nblocks == panels
    loads = loadings.astype(jnp.float32)
    inv_noise = 1.0 / noise_var
    kept_mask = present.astype(jnp.float32)
    weighted = loads * inv_noise[:, None]
    gram_sum = jnp.einsum("bi,is,ir->bsr", kept_mask, weighted, loads, precision=HIGH)
    obs_kept = observed.astype(jnp.float32).reshape(nblocks, BLOCK, series) * kept_mask[:, None, :]
    projected = jnp.dot((obs_kept * inv_noise).reshape(time_rows, series), loads, precision=HIGH)
    persist = 1.0 - decay_rate
    parts = jnp.concatenate([gram_sum, projected.reshape(nblocks, BLOCK, width)], axis=1)
    reduced = scatter_panel(parts)
    pack, powers, partial = local_tables(reduced, persist)
    smoothed = smooth(pack, powers, partial, persist).reshape(time_rows, width)

    total_time = time_rows * segments
    flat_kept = obs_kept.reshape(time_rows, series)
    cross = jnp.dot(smoothed.T, flat_kept, precision=HIGH) / math.sqrt(total_time)
    part = width // panels
    columns = lax.dynamic_slice_in_dim(smoothed, lax.axis_index("panel") * part, part, axis=1)
    moment = jnp.dot(columns.T, smoothed, precision=HIGH) / total_time
    fitted = (
        jnp.dot(smoothed, loads.T, precision=HIGH).reshape(nblocks, BLOCK, series)
        * kept_mask[:, None, :]
    )
    errors = obs_kept - fitted
    square_sums = jnp.sum(errors * errors, axis=(0, 1))
    obs_counts = BLOCK * jnp.sum(kept_mask, axis=0)
    onehot = panel_of_block[:, None] == jnp.arange(128, dtype=jnp.int32)[None, :]
    block_sums = square_sums.reshape(-1, SER_BLOCK).sum(axis=1)
    block_counts = obs_counts.reshape(-1, SER_BLOCK).sum(axis=1)
    sums = jnp.stack(
        [
            jnp.sum(jnp.where(onehot, block_sums[:, None], 0.0), axis=0),
            jnp.sum(jnp.where(onehot, block_counts[:, None], 0.0), axis=0),
        ]
    )
    sums = jnp.concatenate([sums, jnp.zeros((PAD - 2, 128), jnp.float32)], axis=0)
    moment_rows = part * width // segments // 128
    loading_moment, gathered = finish(
        cross.reshape(segments, width // segments, series),
        moment.reshape(segments, moment_rows, 128),
        sums,
    )
    state_moment = gathered[:, :moment_rows].reshape(width, width)
    totals = jnp.sum(gathered[:, moment_rows : moment_rows + 2, :PANELS], axis=0)
    panel_var = totals[0] / jnp.maximum(totals[1], 1.0)
    return (smoothed, loading_moment, state_moment, panel_var)


def solution(mesh):
    return jax.shard_map(
        per_device,
        mesh=mesh,
        in_specs=(
            P("tm", "panel"),
            P("tm", "panel"),
            P("panel", None),
            P("panel"),
            P(),
            P("panel"),
        ),
        out_specs=(P("tm", None), P("tm", "panel"), P(), P()),
        check_vma=False,
    )
```

```python
import functools
import math

import jax
import jax.numpy as jnp
from jax import lax
from jax.experimental import pallas as pl
from jax.experimental.pallas import tpu as pltpu
from jax.sharding import PartitionSpec as P

SER_BLOCK = 128
PANELS = 19
LEVELS = 7
BLOCK = 128
PAD = 8

HIGH = lax.Precision.HIGHEST
MESH = pl.DeviceIdType.MESH
VMEM_LIMIT = 60 * 1024 * 1024


def mm(a, b):
    return jnp.dot(a, b, precision=HIGH, preferred_element_type=jnp.float32)


def mm_t(a, b):
    return lax.dot_general(
        a, b, (((1,), (1,)), ((), ())), precision=HIGH, preferred_element_type=jnp.float32
    )


def vmem(n):
    return [pl.BlockSpec(memory_space=pltpu.VMEM)] * n


def params(collective_id=None):
    if collective_id is None:
        return pltpu.CompilerParams(vmem_limit_bytes=VMEM_LIMIT)
    return pltpu.CompilerParams(
        vmem_limit_bytes=VMEM_LIMIT, collective_id=collective_id, has_side_effects=True
    )


def send_all(axis, n, me, source, target, send, recv):
    def one(d, unused):
        peer = lax.rem(me + d, n)
        pltpu.make_async_remote_copy(
            src_ref=source(peer),
            dst_ref=target(me, d),
            send_sem=send.at[d - 1],
            recv_sem=recv.at[d - 1],
            device_id={axis: peer},
            device_id_type=MESH,
        ).start()
        return unused

    lax.fori_loop(1, n, one, 0)


def wait_all(axis, n, me, source, target, send, recv):
    def one(d, unused):
        origin = lax.rem(me + n - d, n)
        copy = pltpu.make_async_remote_copy(
            src_ref=source(lax.rem(me + d, n)),
            dst_ref=target(origin, d),
            send_sem=send.at[d - 1],
            recv_sem=recv.at[d - 1],
            device_id={axis: origin},
            device_id_type=MESH,
        )
        copy.wait_recv()
        copy.wait_send()
        return unused

    lax.fori_loop(1, n, one, 0)


def greet(groups):
    barrier = pltpu.get_barrier_semaphore()
    total = 0
    for axis, n, me in groups:

        def one(d, unused, axis=axis, n=n, me=me):
            pl.semaphore_signal(
                barrier, inc=1, device_id={axis: lax.rem(me + d, n)}, device_id_type=MESH
            )
            return unused

        lax.fori_loop(1, n, one, 0)
        total += n - 1
    pl.semaphore_wait(barrier, total)


def scatter_kernel(panels, parts, out, landed, send, recv):
    me = lax.axis_index("panel")
    greet([("panel", panels, me)])
    args = ("panel", panels, me, lambda peer: parts.at[peer], lambda i, d: landed.at[d - 1])
    send_all(*args, send, recv)
    total = parts[me]
    wait_all(*args, send, recv)
    for d in range(panels - 1):
        total = total + landed[d]
    out[...] = total


def scatter_panel(parts):
    panels = parts.shape[0]
    shape = parts.shape[1:]
    return pl.pallas_call(
        functools.partial(scatter_kernel, panels),
        out_shape=jax.ShapeDtypeStruct(shape, jnp.float32),
        in_specs=vmem(1),
        out_specs=pl.BlockSpec(memory_space=pltpu.VMEM),
        scratch_shapes=[
            pltpu.VMEM((panels - 1,) + shape, jnp.float32),
            pltpu.SemaphoreType.DMA((panels - 1,)),
            pltpu.SemaphoreType.DMA((panels - 1,)),
        ],
        compiler_params=params(1),
        name="scatter_panel",
    )(parts)


def shift_rows(moved, offset, ahead):
    rows = moved.shape[0]
    zero = jnp.zeros((offset, moved.shape[1]), jnp.float32)
    if offset % 8 == 0:
        if ahead:
            return jnp.concatenate([zero, moved[: rows - offset]], axis=0)
        return jnp.concatenate([moved[offset:], zero], axis=0)
    row = lax.broadcasted_iota(jnp.int32, moved.shape, 0)
    if ahead:
        return jnp.where(row >= offset, pltpu.roll(moved, offset, 0), 0.0)
    return jnp.where(row < rows - offset, pltpu.roll(moved, rows - offset, 0), 0.0)


def unfold(top, corner):
    half = top.shape[0]
    return jnp.concatenate([top, jnp.concatenate([top[:, half:].T, corner], axis=1)], axis=0)


def local_kernel(reduced, rho, rho_row, pack, powers, values_out, stack):
    width = rho.shape[0]
    half = width // 2
    gram = unfold(reduced[:, :width], reduced[:, width : width + half])
    eye = (
        lax.broadcasted_iota(jnp.int32, (width, width), 0)
        == lax.broadcasted_iota(jnp.int32, (width, width), 1)
    ).astype(jnp.float32)
    bound = jnp.max(jnp.sum(jnp.abs(gram), axis=1))
    alpha = 2.0 / (2.0 + bound)
    rest = eye - alpha * (eye + gram)
    stack[:width] = eye + rest
    stack[width:] = mm(rest, rest)
    ratio = bound / (2.0 + bound)

    def step(level):
        grown = mm(stack[...], stack[width:])
        stack[:width] = stack[:width] + grown[:width]
        stack[width:] = grown[width:]
        return level * level

    lax.while_loop(lambda level: level > 1e-5, step, ratio * ratio)
    guess = alpha * stack[:width]
    inverse = guess + mm(guess, (eye - guess) - mm(gram, guess))
    values = mm(reduced[:, width + half :], inverse)
    power = rho[...] * inverse
    for level in range(LEVELS):
        powers[level] = power
        both = mm(jnp.concatenate([power, values], axis=0), power)
        values = values + shift_rows(both[width:], 1 << level, True)
        power = both[:width]
    values_out[...] = values
    scaled = power * rho_row[...]
    pack[:half, :width] = scaled[:half]
    pack[:half, width:] = scaled[half:, half:]
    row = lax.broadcasted_iota(jnp.int32, (PAD, width), 0)
    pack[half:, :width] = jnp.where(row == 0, pltpu.roll(values[BLOCK - PAD :], 1, 0), 0.0)
    pack[half:, width:] = jnp.zeros((PAD, half), jnp.float32)


def local_tables(reduced, persist):
    width = persist.shape[0]
    half = width // 2
    f32 = jnp.float32
    return pl.pallas_call(
        local_kernel,
        out_shape=(
            jax.ShapeDtypeStruct((half + PAD, width + half), f32),
            jax.ShapeDtypeStruct((LEVELS, width, width), f32),
            jax.ShapeDtypeStruct((BLOCK, width), f32),
        ),
        in_specs=vmem(3),
        out_specs=tuple(vmem(3)),
        scratch_shapes=[pltpu.VMEM((2 * width, width), f32)],
        compiler_params=params(),
        name="local_tables",
    )(reduced, persist[:, None], persist[None, :])


def spread(first, powers, ahead):
    rows = mm(first, powers[0])
    if not ahead:
        rows = pltpu.roll(rows, PAD - 1, 0)
    for level in range(LEVELS):
        moved = mm(rows, powers[level])
        if level < 3:
            offset = 1 << level
            rows = rows + pltpu.roll(moved, offset if ahead else PAD - offset, 0)
        elif ahead:
            rows = jnp.concatenate([rows, moved], axis=0)
        else:
            rows = jnp.concatenate([moved, rows], axis=0)
    return rows


def swap(source, target, send, recv, partner):
    return pltpu.make_async_remote_copy(
        src_ref=source,
        dst_ref=target,
        send_sem=send,
        recv_sem=recv,
        device_id={"tm": partner},
        device_id_type=MESH,
    )


def chip_copy(source, target, d, send, recv, chip, chips, core):
    peer = 2 * lax.rem(chip + d, chips) + core
    return swap(source, target, send.at[d - 1], recv.at[d - 1], peer)


def smooth_kernel(
    segments,
    panels,
    pack,
    powers,
    partial,
    rho,
    out,
    landed,
    near,
    far,
    seg_pack,
    pair_in,
    pair_pack,
    own_first,
    firsts,
    seg_first,
    pair_first,
    chip_first,
    chip_firsts,
    mine,
    near_send,
    near_recv,
    pair_send,
    pair_recv,
    far_send,
    far_recv,
):
    width = rho.shape[1]
    half = width // 2
    place = lax.axis_index("panel")
    segment = lax.axis_index("tm")
    chips, chip, core = segments // 2, segment // 2, lax.rem(segment, 2)
    partner = segment + 1 - 2 * core
    greet([("panel", panels, place), ("tm", segments, segment)])

    def gather(source, target, stage):
        args = ("panel", panels, place, lambda peer: source, lambda i, d: target.at[i])
        send_all(*args, near_send.at[stage], near_recv.at[stage])
        target[place] = source[...]
        wait_all(*args, near_send.at[stage], near_recv.at[stage])

    row = lax.broadcasted_iota(jnp.int32, (PAD, width), 0)
    decay = rho[...]
    gather(pack, landed, 0)
    for k in range(panels):
        near[k, :width] = unfold(landed[k, :half, :width], landed[k, :half, width:]) / decay
        near[k, width:] = landed[k, half:, :width]
    whole = near[0]
    keep = (lax.broadcasted_iota(jnp.int32, (width + PAD, width), 0) >= width).astype(jnp.float32)
    for k in range(1, panels):
        whole = mm(whole, near[k, :width]) + keep * near[k]
    seg_pack[...] = whole
    pair = swap(seg_pack, pair_in, pair_send.at[0], pair_recv.at[0], partner)
    pair.start()
    pair.wait()
    first = jnp.where(core == 0, whole, pair_in[...])
    second = jnp.where(core == 0, pair_in[...], whole)
    joined = mm(first, second[:width]) + keep * second
    pair_pack[: width + PAD] = joined
    pair_pack[width + PAD :] = jnp.zeros((PAD, width), jnp.float32)
    share = (width + 2 * PAD) // 2
    rows = pl.ds(pl.multiple_of(core * share, 8), share)

    def out_copy(d, slot):
        return chip_copy(
            pair_pack.at[rows],
            far.at[slot, rows],
            d,
            far_send.at[0],
            far_recv.at[0],
            chip,
            chips,
            core,
        )

    other = pl.ds(pl.multiple_of((1 - core) * share, 8), share)

    def relay(d, part):
        slot = far.at[lax.rem(chip + chips - d, chips), part]
        return swap(slot, slot, far_send.at[1, d - 1], far_recv.at[1, d - 1], partner)

    for d in range(1, chips):
        out_copy(d, chip).start()
    far[chip] = pair_pack[...]
    for d in range(1, chips):
        out_copy(d, lax.rem(chip + chips - d, chips)).wait_recv()
        relay(d, rows).start()
    for d in range(1, chips):
        relay(d, other).wait_recv()
        relay(d, rows).wait_send()
        out_copy(d, chip).wait_send()

    def far_ahead(k, state):
        new = mm(state, far[k, :width]) + far[k, width : width + PAD]
        return jnp.where(k < chip, new, state)

    state = lax.fori_loop(0, chips - 1, far_ahead, jnp.zeros((PAD, width), jnp.float32))
    state = jnp.where(core == 1, mm(state, pair_in[:width]) + pair_in[width:], state)
    for k in range(panels - 1):
        state = jnp.where(k < place, mm(state, near[k, :width]) + near[k, width:], state)

    filtered = partial[...] + spread(state, powers, True)
    values = filtered - mm(filtered * decay, powers[0])
    last = jnp.logical_and(segment == segments - 1, place == panels - 1)
    final_row = lax.broadcasted_iota(jnp.int32, (BLOCK, width), 0) == BLOCK - 1
    values = jnp.where(jnp.logical_and(final_row, last), filtered, values)
    for level in range(LEVELS):
        values = values + shift_rows(mm(values, powers[level]), 1 << level, False)
    own_first[...] = jnp.where(row == 0, values[:PAD], 0.0)
    gather(own_first, firsts, 1)
    total = firsts[panels - 1]
    for k in range(panels - 2, -1, -1):
        total = mm(total, near[k, :width]) + firsts[k]
    total = total * decay
    seg_first[...] = total
    pair = swap(seg_first, pair_first, pair_send.at[1], pair_recv.at[1], partner)
    pair.start()
    pair.wait()
    early = jnp.where(core == 0, total, pair_first[...])
    late = jnp.where(core == 0, pair_first[...], total)
    early_map = jnp.where(core == 0, seg_pack[:width], pair_in[:width])
    both = mm_t(late, early_map) + early
    chip_first[...] = both

    def first_copy(d, slot):
        return chip_copy(
            chip_first,
            chip_firsts.at[slot],
            d,
            far_send.at[2],
            far_recv.at[2],
            chip,
            chips,
            core,
        )

    for d in range(1, chips):
        first_copy(d, chip).start()
    chip_firsts[chip] = both
    for d in range(1, chips):
        first_copy(d, lax.rem(chip + chips - d, chips)).wait_recv()
        first_copy(d, chip).wait_send()

    def far_back(j, state):
        k = chips - 1 - j
        new = mm_t(state, far[k, :width]) + chip_firsts[k]
        return jnp.where(k > chip, new, state)

    state = lax.fori_loop(0, chips - 1, far_back, jnp.zeros((PAD, width), jnp.float32))
    state = jnp.where(core == 0, mm_t(state, pair_in[:width]) + pair_first[...], state)
    state = state / decay
    for k in range(panels - 1, 0, -1):
        state = jnp.where(k > place, mm(state, near[k, :width]) + firsts[k], state)
    mine[...] = values + spread(state, powers, False)
    gather(mine, out, 2)


def smooth(pack, powers, partial, persist):
    width = persist.shape[0]
    segments, panels = lax.axis_size("tm"), lax.axis_size("panel")
    chips = segments // 2
    f32 = jnp.float32
    dma = pltpu.SemaphoreType.DMA
    return pl.pallas_call(
        functools.partial(smooth_kernel, segments, panels),
        out_shape=jax.ShapeDtypeStruct((panels, BLOCK, width), f32),
        in_specs=vmem(4),
        out_specs=pl.BlockSpec(memory_space=pltpu.VMEM),
        scratch_shapes=[
            pltpu.VMEM((panels,) + pack.shape, f32),
            pltpu.VMEM((panels, width + PAD, width), f32),
            pltpu.VMEM((chips, width + 2 * PAD, width), f32),
            pltpu.VMEM((width + PAD, width), f32),
            pltpu.VMEM((width + PAD, width), f32),
            pltpu.VMEM((width + 2 * PAD, width), f32),
            pltpu.VMEM((PAD, width), f32),
            pltpu.VMEM((panels, PAD, width), f32),
            pltpu.VMEM((PAD, width), f32),
            pltpu.VMEM((PAD, width), f32),
            pltpu.VMEM((PAD, width), f32),
            pltpu.VMEM((chips, PAD, width), f32),
            pltpu.VMEM((BLOCK, width), f32),
            dma((3, panels - 1)),
            dma((3, panels - 1)),
            dma((2,)),
            dma((2,)),
            dma((3, chips - 1)),
            dma((3, chips - 1)),
        ],
        compiler_params=params(2),
        name="smooth",
    )(pack, powers, partial, persist[None, :])


def finish_kernel(segments, panels, parts, sums, out, moments, variances, *scratch):
    pair_in, merged, landed, moment, tallies = scratch[:5]
    p_send, p_recv, c_send, c_recv, m_send, m_recv, g_send, g_recv = scratch[5:]
    place = lax.axis_index("panel")
    segment = lax.axis_index("tm")
    chips, chip, core = segments // 2, segment // 2, lax.rem(segment, 2)
    partner = segment + 1 - 2 * core
    devices = segments * panels
    me = place * segments + segment
    series = out.shape[1]
    barrier = pltpu.get_barrier_semaphore()

    def where(d):
        peer = lax.rem(me + d, devices)
        return {"tm": lax.rem(peer, segments), "panel": peer // segments}

    def hello(d, unused):
        pl.semaphore_signal(barrier, inc=1, device_id=where(d), device_id_type=MESH)
        return unused

    lax.fori_loop(1, devices, hello, 0)
    pl.semaphore_wait(barrier, devices - 1)

    pair = swap(parts.at[:, 1 - core], pair_in, p_send.at[0], p_recv.at[0], partner)
    pair.start()

    def tally(d, slot):
        return pltpu.make_async_remote_copy(
            src_ref=sums,
            dst_ref=tallies.at[slot],
            send_sem=g_send.at[d - 1],
            recv_sem=g_recv.at[d - 1],
            device_id=where(d),
            device_id_type=MESH,
        )

    def push(d, unused):
        tally(d, me).start()
        return unused

    lax.fori_loop(1, devices, push, 0)
    tallies[me] = sums[...]
    pair.wait()
    merged[...] = parts[:, core] + pair_in[...]

    def part_copy(d):
        to = lax.rem(chip + d, chips)
        return chip_copy(
            merged.at[to], landed.at[d - 1], d, c_send, c_recv, chip, chips, core
        )

    for d in range(1, chips):
        part_copy(d).start()
    total = merged[chip]
    for d in range(1, chips):
        part_copy(d).wait()
        total = total + landed[d - 1]
    out[...] = total[:, :series]
    moment[...] = total[:, series:]
    args = ("tm", segments, segment, lambda i: moment, lambda i, d: moments.at[i])
    send_all(*args, m_send, m_recv)
    moments[segment] = moment[...]

    def pull(d, unused):
        got = tally(d, lax.rem(me + devices - d, devices))
        got.wait_recv()
        got.wait_send()
        return unused

    lax.fori_loop(1, devices, pull, 0)
    totals = jnp.sum(tallies[...], axis=0)
    variances[...] = totals[0:1] / jnp.maximum(totals[1:2], 1.0)
    wait_all(*args, m_send, m_recv)


def finish(parts, sums, series):
    segments, panels = lax.axis_size("tm"), lax.axis_size("panel")
    devices = segments * panels
    chips = segments // 2
    rows, columns = parts.shape[2:]
    width = columns - series
    f32 = jnp.float32
    dma = pltpu.SemaphoreType.DMA
    return pl.pallas_call(
        functools.partial(finish_kernel, segments, panels),
        out_shape=(
            jax.ShapeDtypeStruct((rows, series), f32),
            jax.ShapeDtypeStruct((segments, rows, width), f32),
            jax.ShapeDtypeStruct((1, 128), f32),
        ),
        in_specs=vmem(2),
        out_specs=tuple(vmem(3)),
        scratch_shapes=[
            pltpu.VMEM((chips, rows, columns), f32),
            pltpu.VMEM((chips, rows, columns), f32),
            pltpu.VMEM((chips - 1, rows, columns), f32),
            pltpu.VMEM((rows, width), f32),
            pltpu.VMEM((devices,) + sums.shape, f32),
            dma((1,)),
            dma((1,)),
            dma((chips - 1,)),
            dma((chips - 1,)),
            dma((segments - 1,)),
            dma((segments - 1,)),
            dma((devices - 1,)),
            dma((devices - 1,)),
        ],
        compiler_params=params(3),
        name="finish",
    )(parts, sums)


def per_device(observed, present, loadings, noise_var, decay_rate, panel_of_block):
    time_rows, series = observed.shape
    width = loadings.shape[1]
    nblocks = time_rows // BLOCK
    segments, panels = lax.axis_size("tm"), lax.axis_size("panel")
    assert nblocks == panels
    loads = loadings.astype(jnp.float32)
    inv_noise = 1.0 / noise_var
    kept_mask = present.astype(jnp.float32)
    weighted = loads * inv_noise[:, None]
    gram_sum = jnp.einsum("bi,is,ir->bsr", kept_mask, weighted, loads, precision=HIGH)
    obs_kept = observed.astype(jnp.float32).reshape(nblocks, BLOCK, series) * kept_mask[:, None, :]
    projected = jnp.dot((obs_kept * inv_noise).reshape(time_rows, series), loads, precision=HIGH)
    persist = 1.0 - decay_rate
    half = width // 2
    parts = jnp.concatenate(
        [
            gram_sum[:, :half],
            gram_sum[:, half:, half:],
            projected.reshape(nblocks, BLOCK, width),
        ],
        axis=2,
    )
    reduced = scatter_panel(parts)
    pack, powers, partial = local_tables(reduced, persist)
    smoothed = smooth(pack, powers, partial, persist).reshape(time_rows, width)

    total_time = time_rows * segments
    flat_kept = obs_kept.reshape(time_rows, series)
    cross = jnp.dot(smoothed.T, flat_kept, precision=HIGH) / math.sqrt(total_time)
    moment = jnp.dot(smoothed.T, smoothed, precision=HIGH) / total_time
    fitted = (
        jnp.dot(smoothed, loads.T, precision=HIGH).reshape(nblocks, BLOCK, series)
        * kept_mask[:, None, :]
    )
    errors = obs_kept - fitted
    square_sums = jnp.sum(errors * errors, axis=(0, 1))
    obs_counts = BLOCK * jnp.sum(kept_mask, axis=0)
    onehot = panel_of_block[:, None] == jnp.arange(128, dtype=jnp.int32)[None, :]
    block_sums = square_sums.reshape(-1, SER_BLOCK).sum(axis=1)
    block_counts = obs_counts.reshape(-1, SER_BLOCK).sum(axis=1)
    sums = jnp.stack(
        [
            jnp.sum(jnp.where(onehot, block_sums[:, None], 0.0), axis=0),
            jnp.sum(jnp.where(onehot, block_counts[:, None], 0.0), axis=0),
        ]
    )
    sums = jnp.concatenate([sums, jnp.zeros((PAD - 2, 128), jnp.float32)], axis=0)
    both = jnp.concatenate([cross, moment], axis=1)
    both = both.reshape(segments // 2, 2, width // segments, series + width)
    loading_moment, moments, variances = finish(both, sums, series)
    state_moment = moments.reshape(width, width)
    panel_var = variances[0, :PANELS]
    return (smoothed, loading_moment, state_moment, panel_var)


def solution(mesh):
    return jax.shard_map(
        per_device,
        mesh=mesh,
        in_specs=(
            P("tm", "panel"),
            P("tm", "panel"),
            P("panel", None),
            P("panel"),
            P(),
            P("panel"),
        ),
        out_specs=(P("tm", None), P("tm", "panel"), P(), P()),
        check_vma=False,
    )
```
